32 devices in a mesh: gx: 4 (over x, core), gy: 2 (over y), gz: 4 (over z).
Axes of the slice: x: 2, y: 2, z: 4, core: 2. Of those that a mesh axis runs over, the one named last changes fastest.
Arguments:
- node_feats: bfloat16 [64, 32, 128, 128], P('gx', 'gy', 'gz'), may hold values from -6 to 6
- node_type: int32 [64, 32, 128], P('gx', 'gy', 'gz'), may hold values from 0 to 3
- boundary_code: int32 [64, 32, 128], P('gx', 'gy', 'gz'), may hold values from 0 to 2
- wall_flag: int32 [64, 32, 128], P('gx', 'gy', 'gz'), may hold values from 0 to 1, as said below
- type_table: float32 [4, 128], replicated, may hold values from -3 to 3
- boundary_table: float32 [3, 128], replicated, may hold values from -3 to 3
- edge_self: bfloat16 [2, 128, 128], replicated, may hold values from -0.5 to 0.5
- edge_neighbour: bfloat16 [2, 128, 128], replicated, may hold values from -0.5 to 0.5
- edge_bias: float32 [2, 6, 128], replicated, may hold values from -3 to 3
- edge_out: bfloat16 [2, 128, 128], replicated, may hold values from -0.5 to 0.5
- node_self: bfloat16 [2, 128, 128], replicated, may hold values from -0.5 to 0.5
- node_aggregate: bfloat16 [2, 128, 128], replicated, may hold values from -0.5 to 0.5
- node_out: bfloat16 [2, 128, 128], replicated, may hold values from -0.5 to 0.5
- node_gain: float32 [2, 128], replicated, may hold values from 0.25 to 1.75
Outputs:
- latent: bfloat16 [64, 32, 128, 128], P('gx', 'gy', 'gz')
- wall_mean: float32 [128], replicated
The draws below stay inside these ranges and needn't reach their ends.
Inputs may be any that keep to these rules, and one draw needn't show every extreme that they name: Every node whose wall-normal index is 0 or 31 has wall_flag 1.
All inputs are finite; a program needn't handle non-finite values.
Results may differ from the reference program's by a relative error of at most 0.012.
Values may be sent and summed in bfloat16 or wider, within the bound.
A program may use at most 128 MiB of HBM per device.

```python
import jax
import jax.numpy as jnp
from jax import lax

H = 128
LAYERS = 2
NTYPES = 4
NCODES = 3
NX = 64
NY = 32
NZ = 128


def draw_wall_flag(key, part):
    picks = jax.random.randint(jax.random.fold_in(key, 17), (NX, NY, NZ), 0, 8)
    rows_y = jnp.arange(NY, dtype=jnp.int32)[None, :, None]
    on_wall = jnp.logical_or(rows_y == 0, rows_y == NY - 1)
    flagged = jnp.logical_or(picks == 0, on_wall)
    return flagged.astype(jnp.int32)


def plant(array, own_key, least, largest):
    shape = array.shape
    spot = [jax.random.randint(jax.random.fold_in(own_key, axis), (), 0, shape[axis]) for axis in range(len(shape))]
    array = array.at[tuple(spot)].set(least)
    longest = shape.index(max(shape))
    spot[longest] = (spot[longest] + 1) % shape[longest]
    return array.at[tuple(spot)].set(largest)


def block_levels(key, extent, cuts, smallest, high):
    def one(dim, parts):
        draws = jax.random.uniform(jax.random.fold_in(jax.random.fold_in(key, 6), dim), (parts,), jnp.float32, smallest / len(cuts), high / len(cuts))
        return jnp.repeat(jnp.exp(draws), extent[dim] // parts).reshape((-1,) + (1,) * (len(extent) - dim - 1))

    gain = one(*cuts[0])
    for cut in cuts[1:]:
        gain = gain * one(*cut)
    return gain


def scatter_about(key, shape, scale, reach, pieces=(), held_as=jnp.bfloat16):
    level = block_levels(key, shape, pieces, -0.22, 0.18) if pieces else 1.0
    entries = jax.random.normal(key, shape, jnp.float32) * scale * level
    return jnp.minimum(jnp.maximum(entries, -reach), reach).astype(held_as)


def setup_inputs(seed: int = 0) -> dict:
    splits = jax.random.split(jax.random.key(seed), 15)
    return {
        "node_feats": scatter_about(splits[0], (NX, NY, NZ, H), 1.0, 6.0, ((0, 4), (1, 2), (2, 4))),
        "node_type": plant(jax.random.randint(splits[1], (NX, NY, NZ), 0, NTYPES), jax.random.fold_in(splits[1], 1), 0, NTYPES - 1).astype(jnp.int32),
        "boundary_code": plant(jax.random.randint(splits[2], (NX, NY, NZ), 0, NCODES), jax.random.fold_in(splits[2], 1), 0, NCODES - 1).astype(jnp.int32),
        "wall_flag": draw_wall_flag(jax.random.fold_in(splits[14], 71), 0),
        "type_table": scatter_about(splits[4], (NTYPES, H), 0.5, 3.0, (), jnp.float32),
        "boundary_table": scatter_about(splits[5], (NCODES, H), 0.5, 3.0, (), jnp.float32),
        "edge_self": scatter_about(splits[6], (LAYERS, H, H), H ** -0.5, 0.5),
        "edge_neighbour": scatter_about(splits[7], (LAYERS, H, H), H ** -0.5, 0.5),
        "edge_bias": scatter_about(splits[8], (LAYERS, 6, H), 0.5, 3.0, (), jnp.float32),
        "edge_out": scatter_about(splits[9], (LAYERS, H, H), H ** -0.5, 0.5),
        "node_self": scatter_about(splits[10], (LAYERS, H, H), H ** -0.5, 0.5),
        "node_aggregate": scatter_about(splits[11], (LAYERS, H, H), H ** -0.5, 0.5),
        "node_out": scatter_about(splits[12], (LAYERS, H, H), H ** -0.5, 0.5),
        "node_gain": jnp.clip(1.0 + 0.15 * jax.random.normal(splits[13], (LAYERS, H), jnp.float32), 0.25, 1.75),
    }


epsilon = 1e-05

def reference(node_feats, node_type, boundary_code, wall_flag, type_table, boundary_table, edge_self, edge_neighbour, edge_bias, edge_out, node_self, node_aggregate, node_out, node_gain):
    latent = (node_feats.astype(jnp.float32) + type_table[node_type] + boundary_table[boundary_code]).astype(jnp.bfloat16)
    rows_y = jnp.arange(NY)
    lower_ok = (rows_y >= 1).astype(jnp.float32)[None, :, None, None]
    upper_ok = (rows_y < NY - 1).astype(jnp.float32)[None, :, None, None]
    for which_layer in range(LAYERS):
        selfpart = jnp.dot(latent, edge_self[which_layer], preferred_element_type=jnp.float32)
        sendpart = jnp.dot(latent, edge_neighbour[which_layer], preferred_element_type=jnp.float32).astype(jnp.bfloat16)
        shifts = [(1, 0), (-1, 0), (1, 1), (-1, 1), (1, 2), (-1, 2)]
        masks = [None, None, lower_ok, upper_ok, None, None]
        aggregate = jnp.zeros(selfpart.shape, jnp.float32)
        for direction in range(6):
            neighbour = jnp.roll(sendpart, shifts[direction][0], axis=shifts[direction][1])
            hidden = jax.nn.silu(selfpart + neighbour.astype(jnp.float32) + edge_bias[which_layer, direction]).astype(jnp.bfloat16)
            message = jnp.dot(hidden, edge_out[which_layer], preferred_element_type=jnp.float32)
            if masks[direction] is not None:
                message = message * masks[direction]
            aggregate = aggregate + message
        aggregate = aggregate.astype(jnp.bfloat16)
        before = jnp.dot(latent, node_self[which_layer], preferred_element_type=jnp.float32) + jnp.dot(aggregate, node_aggregate[which_layer], preferred_element_type=jnp.float32)
        inner = jax.nn.silu(before).astype(jnp.bfloat16)
        update = jnp.dot(inner, node_out[which_layer], preferred_element_type=jnp.float32)
        centre = lax.optimization_barrier(jnp.mean(update, axis=-1, keepdims=True))
        spread = lax.optimization_barrier(jnp.mean(jnp.square(update - centre), axis=-1, keepdims=True))
        normed = (update - centre) * jax.lax.rsqrt(spread + epsilon) * node_gain[which_layer]
        latent = (latent.astype(jnp.float32) + normed).astype(jnp.bfloat16)
    flags = wall_flag.astype(jnp.float32)
    wall_sum = lax.optimization_barrier(jnp.sum(latent.astype(jnp.float32) * flags[..., None], axis=(0, 1, 2)))
    wall_count = jnp.sum(flags)
    return (latent, wall_sum / wall_count)
```

```python
import functools

import jax
import jax.numpy as jnp
from jax import lax
from jax.experimental import pallas as pl
from jax.experimental.pallas import tpu as pltpu
from jax.sharding import PartitionSpec as P

epsilon = 1e-05
PAD = 8
F32 = jnp.float32
BF16 = jnp.bfloat16


def dot(a, b):
    return jnp.dot(a, b, preferred_element_type=F32)


def gated(u):
    return u * (1.0 + jnp.tanh(u))


def kernel(
    sizes,
    feats, code, type_table, boundary_table, edge_self, edge_neighbour, edge_bias, edge_out,
    node_self, node_aggregate, node_out, node_gain,
    out, wall_out,
    fbuf, lat, spart, npart, hsum, hbf, table,
    wcat, wnode, wout,
    xsend, xrecv, ysend, yrecv, zsend, zrecv,
    wall, redx, redy, redz,
    fsem, osem, hsend_sem, hrecv_sem, rsend_sem, rrecv_sem,
):
    X, Y, Z, H, L, gx, gy, gz = sizes
    ZP = Z + 2 * PAD
    R = Y * Z
    counts = {"gx": gx, "gy": gy, "gz": gz}
    me = {a: lax.axis_index(a) for a in counts}

    def load_feats(x):
        return pltpu.make_async_copy(feats.at[x], fbuf.at[x], fsem.at[x])

    for x in range(X):
        load_feats(x).start()

    barrier = pltpu.get_barrier_semaphore()
    total = 0
    for a, n in counts.items():
        for k in range(1, n):
            peer = lax.rem(me[a] + k, n)
            pl.semaphore_signal(
                barrier, inc=1, device_id={a: peer}, device_id_type=pl.DeviceIdType.MESH
            )
            total += 1

    for l in range(L):
        wcat[l, :, :H] = (edge_self[l].astype(F32) * 0.5).astype(BF16)
        wcat[l, :, H:] = (edge_neighbour[l].astype(F32) * 0.5).astype(BF16)
        wnode[l, :H] = (node_self[l].astype(F32) * 0.5).astype(BF16)
        wnode[l, H:] = (dot(edge_out[l], node_aggregate[l]) * 0.5).astype(BF16)
        w = node_out[l].astype(F32)
        wout[l] = (w - jnp.mean(w, axis=-1, keepdims=True)).astype(BF16)
    ones = jnp.full((H, H), 1.0 / H, BF16)

    NT, NC = type_table.shape[0], boundary_table.shape[0]
    KT = NT * NC
    KP = table.shape[0]
    table[...] = jnp.zeros_like(table)
    for i in range(NT):
        table[i * NC:(i + 1) * NC] = boundary_table[...] + type_table[i:i + 1]
    t = table[...]
    hi = t.astype(BF16)
    rest = t - hi.astype(F32)
    mid = rest.astype(BF16)
    low = (rest - mid.astype(F32)).astype(BF16)
    table3 = jnp.concatenate([hi, mid, low], axis=0)

    def start_latent(x):
        load_feats(x).wait()
        c = code[x]
        c = jnp.where(c >= KT, c - KT, c)
        rows = lax.broadcasted_iota(jnp.int32, (KP, R), 0)
        hot = jnp.where(rows == c, 1.0, 0.0).astype(BF16)
        hot3 = jnp.concatenate([hot, hot, hot], axis=0)
        extra = lax.dot_general(
            hot3, table3, (((0,), (0,)), ((), ())), preferred_element_type=F32
        )
        lat[x] = (fbuf[x].astype(F32) + extra).astype(BF16)

    def loop(lo, hi, fn):
        def body(i, carry):
            fn(i)
            return carry
        lax.fori_loop(lo, hi, body, 0)

    def halo(l, slot, src, dst, axis, peer):
        return pltpu.make_async_remote_copy(
            src_ref=src,
            dst_ref=dst,
            send_sem=hsend_sem.at[l, slot],
            recv_sem=hrecv_sem.at[l, slot],
            device_id={axis: peer},
            device_id_type=pl.DeviceIdType.MESH,
        )

    up = {a: lax.rem(me[a] + 1, n) for a, n in counts.items()}
    down = {a: lax.rem(me[a] + n - 1, n) for a, n in counts.items()}
    wall[...] = jnp.zeros_like(wall)

    for l in range(L):
        last = l == L - 1
        xs = [
            halo(l, 0, xsend.at[l, 1], xrecv.at[l, 0], "gx", up["gx"]),
            halo(l, 1, xsend.at[l, 0], xrecv.at[l, 1], "gx", down["gx"]),
        ]
        zs = [
            halo(l, 2, zsend.at[l, 1], zrecv.at[l, 0], "gz", up["gz"]),
            halo(l, 3, zsend.at[l, 0], zrecv.at[l, 1], "gz", down["gz"]),
        ]
        y_up = halo(l, 4, ysend.at[l, 1], yrecv.at[l, 0], "gy", up["gy"])
        y_down = halo(l, 5, ysend.at[l, 0], yrecv.at[l, 1], "gy", down["gy"])
        has_low = me["gy"] > 0
        has_high = me["gy"] < gy - 1

        def project(x, face=None, l=l):
            if l == 0:
                start_latent(x)
            p = dot(lat[x], wcat[l])
            spart[x] = p[:, :H]
            n = p[:, H:]
            for y in range(Y):
                npart[x + 1, y * ZP + PAD:y * ZP + PAD + Z] = n[y * Z:(y + 1) * Z]
            if face is not None:
                xsend[l, face] = n.astype(BF16)
            ysend[l, 0, x] = n[:Z].astype(BF16)
            ysend[l, 1, x] = n[R - Z:].astype(BF16)
            zsend[l, 0, x] = npart[x + 1, pl.ds(PAD, Y, stride=ZP), :].astype(BF16)
            zsend[l, 1, x] = npart[x + 1, pl.ds(PAD + Z - 1, Y, stride=ZP), :].astype(BF16)

        project(0, 0)
        project(X - 1, 1)
        if l == 0:
            pl.semaphore_wait(barrier, total)
        for c in xs:
            c.start()
        loop(1, X - 1, project)
        for c in zs:
            c.start()
        pl.when(has_high)(y_up.start)
        pl.when(has_low)(y_down.start)

        bias = [edge_bias[l, d:d + 1] * 0.5 for d in range(6)]

        def neighbour(x, y, dz=0):
            return npart[x, pl.ds(y * ZP + PAD + dz, Z), :]

        def edges_xy(x):
            for y in range(Y):
                s = spart[x, y * Z:(y + 1) * Z]
                h = gated(s + neighbour(x, y) + bias[0]) + gated(s + neighbour(x + 2, y) + bias[1])
                if y > 0:
                    h = h + gated(s + neighbour(x + 1, y - 1) + bias[2])
                if y < Y - 1:
                    h = h + gated(s + neighbour(x + 1, y + 1) + bias[3])
                hsum[x, y * Z:(y + 1) * Z] = h

        loop(1, X - 1, edges_xy)

        for c in xs:
            c.wait()
        for side, slab in ((0, 0), (1, X + 1)):
            for y in range(Y):
                npart[slab, y * ZP + PAD:y * ZP + PAD + Z] = xrecv[l, side, y * Z:(y + 1) * Z].astype(F32)
        loop(0, 2, lambda i: edges_xy(i * (X - 1)))

        @pl.when(has_low)
        def _():
            y_up.wait_recv()

            def add(x):
                s = spart[x, :Z]
                hsum[x, :Z] = hsum[x, :Z] + gated(s + yrecv[l, 0, x].astype(F32) + bias[2])

            loop(0, X, add)

        @pl.when(has_high)
        def _():
            y_down.wait_recv()

            def add(x):
                s = spart[x, R - Z:]
                hsum[x, R - Z:] = hsum[x, R - Z:] + gated(s + yrecv[l, 1, x].astype(F32) + bias[3])

            loop(0, X, add)

        pl.when(has_high)(y_up.wait_send)
        pl.when(has_low)(y_down.wait_send)
        for c in zs:
            c.wait()

        def edges_z(x):
            npart[x + 1, pl.ds(PAD - 1, Y, stride=ZP), :] = zrecv[l, 0, x].astype(F32)
            npart[x + 1, pl.ds(PAD + Z, Y, stride=ZP), :] = zrecv[l, 1, x].astype(F32)
            for y in range(Y):
                rows = slice(y * Z, (y + 1) * Z)
                s = spart[x, rows]
                h = hsum[x, rows]
                h = h + gated(s + neighbour(x + 1, y, -1) + bias[4])
                h = h + gated(s + neighbour(x + 1, y, 1) + bias[5])
                hbf[x, rows] = h.astype(BF16)

        loop(0, X, edges_z)

        gain = node_gain[l:l + 1]

        def store(x):
            return pltpu.make_async_copy(lat.at[x], out.at[x], osem.at[x])

        def nodes(x, l=l, last=last):
            news = []
            B = R // 2
            for b in range(0, R, B):
                old = lat[x, b:b + B]
                u = dot(jnp.concatenate([old, hbf[x, b:b + B]], axis=1), wnode[l])
                inner = gated(u).astype(BF16)
                upd = dot(inner, wout[l])
                var = dot((upd * upd).astype(BF16), ones)
                new = old.astype(F32) + upd * lax.rsqrt(var + epsilon) * gain
                news.append(new.astype(BF16))
            for i, new in enumerate(news):
                lat[x, i * B:(i + 1) * B] = new
            if last:
                store(x).start()
                flag = jnp.where(code[x] >= KT, 1.0, 0.0)
                flag = jnp.broadcast_to(flag, (16, R)).astype(BF16)
                new = jnp.concatenate(news, axis=0)
                wide = jnp.concatenate([new, jnp.ones((R, H), BF16)], axis=1)
                wall[...] += dot(flag, wide)

        loop(0, X, nodes)

    part = wall[:8]
    for index, (a, red) in enumerate((("gx", redx), ("gy", redy), ("gz", redz))):
        n = counts[a]
        red[me[a]] = part
        copies = []
        for k in range(1, n):
            copies.append(pltpu.make_async_remote_copy(
                src_ref=red.at[me[a]],
                dst_ref=red.at[me[a]],
                send_sem=rsend_sem.at[index, k],
                recv_sem=rrecv_sem.at[index, k],
                device_id={a: lax.rem(me[a] + k, n)},
                device_id_type=pl.DeviceIdType.MESH,
            ))
        for c in copies:
            c.start()
        for c in copies:
            c.wait()
        part = red[0]
        for i in range(1, n):
            part = part + red[i]
    wall_out[...] = part[:1, :H] / part[:1, H:]
    loop(0, X, lambda x: store(x).wait())


def per_device(
    node_feats,
    node_type,
    boundary_code,
    wall_flag,
    type_table,
    boundary_table,
    edge_self,
    edge_neighbour,
    edge_bias,
    edge_out,
    node_self,
    node_aggregate,
    node_out,
    node_gain,
):
    X, Y, Z, H = node_feats.shape
    L = edge_self.shape[0]
    gx, gy, gz = (lax.axis_size(a) for a in ("gx", "gy", "gz"))
    NT, NC = type_table.shape[0], boundary_table.shape[0]
    R, ZP = Y * Z, Z + 2 * PAD
    most = max(gx, gy, gz)
    code = (node_type * NC + boundary_code + wall_flag * (NT * NC)).reshape(X, 1, R)
    vmem = pl.BlockSpec(memory_space=pltpu.VMEM)
    hbm = pl.BlockSpec(memory_space=pl.ANY)
    latent, wall_mean = pl.pallas_call(
        functools.partial(kernel, (X, Y, Z, H, L, gx, gy, gz)),
        out_shape=(
            jax.ShapeDtypeStruct((X, R, H), BF16),
            jax.ShapeDtypeStruct((1, H), F32),
        ),
        in_specs=[hbm] + [vmem] * 11,
        out_specs=(hbm, vmem),
        scratch_shapes=[
            pltpu.VMEM((X, R, H), BF16),
            pltpu.VMEM((X, R, H), BF16),
            pltpu.VMEM((X, R, H), F32),
            pltpu.VMEM((X + 2, Y * ZP, H), F32),
            pltpu.VMEM((X, R, H), F32),
            pltpu.VMEM((X, R, H), BF16),
            pltpu.VMEM((pl.cdiv(NT * NC, 16) * 16, H), F32),
            pltpu.VMEM((L, H, 2 * H), BF16),
            pltpu.VMEM((L, 2 * H, H), BF16),
            pltpu.VMEM((L, H, H), BF16),
            pltpu.VMEM((L, 2, R, H), BF16),
            pltpu.VMEM((L, 2, R, H), BF16),
            pltpu.VMEM((L, 2, X, Z, H), BF16),
            pltpu.VMEM((L, 2, X, Z, H), BF16),
            pltpu.VMEM((L, 2, X, Y, H), BF16),
            pltpu.VMEM((L, 2, X, Y, H), BF16),
            pltpu.VMEM((16, 2 * H), F32),
            pltpu.VMEM((gx, 8, 2 * H), F32),
            pltpu.VMEM((gy, 8, 2 * H), F32),
            pltpu.VMEM((gz, 8, 2 * H), F32),
            pltpu.SemaphoreType.DMA((X,)),
            pltpu.SemaphoreType.DMA((X,)),
            pltpu.SemaphoreType.DMA((L, 6)),
            pltpu.SemaphoreType.DMA((L, 6)),
            pltpu.SemaphoreType.DMA((3, most)),
            pltpu.SemaphoreType.DMA((3, most)),
        ],
        compiler_params=pltpu.CompilerParams(collective_id=0, has_side_effects=True),
        name="mesh_step",
    )(
        node_feats.reshape(X, R, H), code, type_table, boundary_table, edge_self, edge_neighbour,
        edge_bias, edge_out, node_self, node_aggregate, node_out, node_gain,
    )
    return latent.reshape(X, Y, Z, H), wall_mean.reshape(H)


def solution(mesh):
    return jax.shard_map(
        per_device,
        mesh=mesh,
        in_specs=(
            P("gx", "gy", "gz", None),
            P("gx", "gy", "gz"),
            P("gx", "gy", "gz"),
            P("gx", "gy", "gz"),
            P(),
            P(),
            P(),
            P(),
            P(),
            P(),
            P(),
            P(),
            P(),
            P(),
        ),
        out_specs=(P("gx", "gy", "gz", None), P()),
        check_vma=False,
    )
```

```python
import functools

import jax
import jax.numpy as jnp
from jax import lax
from jax.experimental import pallas as pl
from jax.experimental.pallas import tpu as pltpu
from jax.sharding import PartitionSpec as P

epsilon = 1e-05
PAD = 8
F32 = jnp.float32
BF16 = jnp.bfloat16


def dot(a, b):
    return jnp.dot(a, b, preferred_element_type=F32)


def gated(u):
    return u * (1.0 + jnp.tanh(u))


def kernel(
    sizes,
    feats, code, type_table, boundary_table, edge_self, edge_neighbour, edge_bias, edge_out,
    node_self, node_aggregate, node_out, node_gain,
    out, wall_out,
    fbuf, lat, spart, npart, hsum, hbf, pre, upd, table,
    wcat, wnode, wout,
    xsend, xrecv, ysend, yrecv, zsend, zrecv,
    wall, redxy, redz,
    fsem, osem, hsend_sem, hrecv_sem, rsend_sem, rrecv_sem,
):
    X, Y, Z, H, L, gx, gy, gz = sizes
    ZP = Z + 2 * PAD
    R = Y * Z
    counts = {"gx": gx, "gy": gy, "gz": gz}
    me = {a: lax.axis_index(a) for a in counts}

    def load_feats(x):
        return pltpu.make_async_copy(feats.at[x], fbuf.at[x], fsem.at[x])

    for x in range(X):
        load_feats(x).start()

    def plane(k):
        return {"gx": lax.rem(me["gx"] + k // gy, gx), "gy": lax.rem(me["gy"] + k % gy, gy)}

    def line(k):
        return {"gz": lax.rem(me["gz"] + k, gz)}

    barrier = pltpu.get_barrier_semaphore()
    peers = [plane(k) for k in range(1, gx * gy)] + [line(k) for k in range(1, gz)]
    total = len(peers)
    for peer in peers:
        pl.semaphore_signal(
            barrier, inc=1, device_id=peer, device_id_type=pl.DeviceIdType.MESH
        )

    for l in range(L):
        wcat[l, :, :H] = (edge_self[l].astype(F32) * 0.5).astype(BF16)
        wcat[l, :, H:] = (edge_neighbour[l].astype(F32) * 0.5).astype(BF16)
        wnode[l, :H] = (node_self[l].astype(F32) * 0.5).astype(BF16)
        wnode[l, H:] = (dot(edge_out[l], node_aggregate[l]) * 0.5).astype(BF16)
        w = node_out[l].astype(F32)
        wout[l] = (w - jnp.mean(w, axis=-1, keepdims=True)).astype(BF16)
    ones = jnp.full((H, H), 1.0 / H, BF16)

    NT, NC = type_table.shape[0], boundary_table.shape[0]
    KT = NT * NC
    KP = table.shape[0]
    table[...] = jnp.zeros_like(table)
    for i in range(NT):
        table[i * NC:(i + 1) * NC] = boundary_table[...] + type_table[i:i + 1]
    t = table[...]
    hi = t.astype(BF16)
    rest = t - hi.astype(F32)
    mid = rest.astype(BF16)
    low = (rest - mid.astype(F32)).astype(BF16)
    table3 = jnp.concatenate([hi, mid, low], axis=0)

    def start_latent(x):
        load_feats(x).wait()
        c = code[x]
        c = jnp.where(c >= KT, c - KT, c)
        rows = lax.broadcasted_iota(jnp.int32, (KP, R), 0)
        hot = jnp.where(rows == c, 1.0, 0.0).astype(BF16)
        hot3 = jnp.concatenate([hot, hot, hot], axis=0)
        extra = lax.dot_general(
            hot3, table3, (((0,), (0,)), ((), ())), preferred_element_type=F32
        )
        lat[x] = (fbuf[x].astype(F32) + extra).astype(BF16)

    def loop(lo, hi, fn):
        def body(i, carry):
            fn(i)
            return carry
        lax.fori_loop(lo, hi, body, 0)

    def halo(l, slot, src, dst, axis, peer):
        return pltpu.make_async_remote_copy(
            src_ref=src,
            dst_ref=dst,
            send_sem=hsend_sem.at[l, slot],
            recv_sem=hrecv_sem.at[l, slot],
            device_id={axis: peer},
            device_id_type=pl.DeviceIdType.MESH,
        )

    up = {a: lax.rem(me[a] + 1, n) for a, n in counts.items()}
    down = {a: lax.rem(me[a] + n - 1, n) for a, n in counts.items()}
    wall[...] = jnp.zeros_like(wall)

    for l in range(L):
        last = l == L - 1
        has_low = me["gy"] > 0
        has_high = me["gy"] < gy - 1
        xs = [
            halo(l, 0, xsend.at[l, 1], xrecv.at[l, 0], "gx", up["gx"]),
            halo(l, 1, xsend.at[l, 0], xrecv.at[l, 1], "gx", down["gx"]),
        ]
        zs = [
            halo(l, 2, zsend.at[l, 1], zrecv.at[l, 0], "gz", up["gz"]),
            halo(l, 3, zsend.at[l, 0], zrecv.at[l, 1], "gz", down["gz"]),
        ]
        y_up = halo(l, 4, ysend.at[l, 1], yrecv.at[l, 0], "gy", up["gy"])
        y_down = halo(l, 5, ysend.at[l, 0], yrecv.at[l, 1], "gy", down["gy"])

        def project(x, face=None, l=l):
            p = dot(lat[x], wcat[l])
            spart[x] = p[:, :H]
            n = p[:, H:]
            for y in range(Y):
                npart[x + 1, y * ZP + PAD:y * ZP + PAD + Z] = n[y * Z:(y + 1) * Z]
            if face is not None:
                xsend[l, face] = n.astype(BF16)
            ysend[l, 0, x] = n[:Z].astype(BF16)
            ysend[l, 1, x] = n[R - Z:].astype(BF16)
            zsend[l, 0, x] = npart[x + 1, pl.ds(PAD, Y, stride=ZP), :].astype(BF16)
            zsend[l, 1, x] = npart[x + 1, pl.ds(PAD + Z - 1, Y, stride=ZP), :].astype(BF16)

        if l == 0:
            start_latent(0)

            def ahead(x):
                project(x)
                start_latent(x + 1)

            project(0, 0)
            start_latent(1)
            loop(1, X - 1, ahead)
            project(X - 1, 1)
            pl.semaphore_wait(barrier, total)
            for c in xs:
                c.start()
        else:
            project(0, 0)
            project(X - 1, 1)
            for c in xs:
                c.start()
            loop(1, X - 1, project)
        pl.when(has_high)(y_up.start)
        pl.when(has_low)(y_down.start)
        for c in zs:
            c.start()

        bias = [(edge_bias[d, l:l + 1] * 0.5).astype(BF16) for d in range(6)]

        def neighbour(x, y, dz=0):
            return npart[x, pl.ds(y * ZP + PAD + dz, Z), :].astype(BF16)

        def edges_xy(x, l=l, bias=bias):
            for y in range(Y):
                rows = slice(y * Z, (y + 1) * Z)
                s = spart[x, rows].astype(BF16)
                h = gated(s + neighbour(x, y) + bias[0]) + gated(s + neighbour(x + 2, y) + bias[1])
                if y > 0:
                    h = h + gated(s + neighbour(x + 1, y - 1) + bias[2])
                if y < Y - 1:
                    h = h + gated(s + neighbour(x + 1, y + 1) + bias[3])
                hsum[x, rows] = h.astype(F32)

        loop(1, X - 1, edges_xy)
        for c in xs:
            c.wait()
        for side, slab in ((0, 0), (1, X + 1)):
            for y in range(Y):
                npart[slab, y * ZP + PAD:y * ZP + PAD + Z] = xrecv[l, side, y * Z:(y + 1) * Z].astype(F32)
        loop(0, 2, lambda i: edges_xy(i * (X - 1)))

        def edge_rows(face, first, d, l=l, bias=bias):
            def add(x):
                rows = slice(first, first + Z)
                u = spart[x, rows] + yrecv[l, face, x].astype(F32) + edge_bias[d, l:l + 1] * 0.5
                hsum[x, rows] = hsum[x, rows] + gated(u)

            loop(0, X, add)

        @pl.when(has_low)
        def _():
            y_up.wait_recv()
            edge_rows(0, 0, 2)

        @pl.when(has_high)
        def _():
            y_down.wait_recv()
            edge_rows(1, R - Z, 3)

        pl.when(has_high)(y_up.wait_send)
        pl.when(has_low)(y_down.wait_send)
        for c in zs:
            c.wait()

        def edges_z(x, l=l, bias=bias):
            npart[x + 1, pl.ds(PAD - 1, Y, stride=ZP), :] = zrecv[l, 0, x].astype(F32)
            npart[x + 1, pl.ds(PAD + Z, Y, stride=ZP), :] = zrecv[l, 1, x].astype(F32)
            for y in range(Y):
                rows = slice(y * Z, (y + 1) * Z)
                s = spart[x, rows].astype(BF16)
                h = gated(s + neighbour(x + 1, y, -1) + bias[4])
                h = h + gated(s + neighbour(x + 1, y, 1) + bias[5])
                hbf[x, rows] = h + hsum[x, rows].astype(BF16)

        gain = node_gain[l:l + 1]

        def store(x):
            return pltpu.make_async_copy(lat.at[x], out.at[x], osem.at[x])

        def first_layer(x, l=l):
            pre[...] = dot(jnp.concatenate([lat[x], hbf[x]], axis=1), wnode[l])

        def second_layer(l=l):
            upd[...] = dot(gated(pre[...]).astype(BF16), wout[l])

        def finish(x, last=last, gain=gain):
            change = upd[...]
            var = dot((change * change).astype(BF16), ones)
            new = lat[x].astype(F32) + change * lax.rsqrt(var + epsilon) * gain
            new = new.astype(BF16)
            lat[x] = new
            if last:
                flag = jnp.where(code[x] >= KT, 1.0, 0.0)
                flag = jnp.broadcast_to(flag, (16, R)).astype(BF16)
                wide = jnp.concatenate([new, jnp.ones((R, H), BF16)], axis=1)
                wall[...] += dot(flag, wide)

        def step(x, edge, one, two, three, last=last):
            if three:
                finish(x - 3)
            if two:
                second_layer()
            if one:
                first_layer(x - 1)
            if edge:
                edges_z(x)
            if three and last:
                store(x - 3).start()

        step(0, True, False, False, False)
        step(1, True, True, False, False)
        step(2, True, True, True, False)
        loop(3, X, lambda x, step=step: step(x, True, True, True, True))
        step(X, False, True, True, True)
        step(X + 1, False, False, True, True)
        step(X + 2, False, False, False, True)

    def exchange(part, red, index, mine, count, place):
        red[mine] = part
        copies = []
        for k in range(1, count):
            copies.append(pltpu.make_async_remote_copy(
                src_ref=red.at[mine],
                dst_ref=red.at[mine],
                send_sem=rsend_sem.at[index, k],
                recv_sem=rrecv_sem.at[index, k],
                device_id=place(k),
                device_id_type=pl.DeviceIdType.MESH,
            ))
        for c in copies:
            c.start()
        for c in copies:
            c.wait()
        total = red[0]
        for i in range(1, count):
            total = total + red[i]
        return total

    first = lax.broadcasted_iota(jnp.int32, (8, H), 0) == 0
    part = jnp.where(first, wall[:8, :H], wall[:8, H:])
    part = exchange(part, redxy, 0, me["gx"] * gy + me["gy"], gx * gy, plane)
    part = exchange(part, redz, 1, me["gz"], gz, line)
    wall_out[...] = part[:1] / part[1:2]
    loop(0, X, lambda x: store(x).wait())


def per_device(
    node_feats,
    node_type,
    boundary_code,
    wall_flag,
    type_table,
    boundary_table,
    edge_self,
    edge_neighbour,
    edge_bias,
    edge_out,
    node_self,
    node_aggregate,
    node_out,
    node_gain,
):
    X, Y, Z, H = node_feats.shape
    L = edge_self.shape[0]
    gx, gy, gz = (lax.axis_size(a) for a in ("gx", "gy", "gz"))
    NT, NC = type_table.shape[0], boundary_table.shape[0]
    R, ZP = Y * Z, Z + 2 * PAD
    most = max(gx * gy, gz)
    code = (node_type * NC + boundary_code + wall_flag * (NT * NC)).reshape(X, 1, R)
    vmem = pl.BlockSpec(memory_space=pltpu.VMEM)
    hbm = pl.BlockSpec(memory_space=pl.ANY)
    latent, wall_mean = pl.pallas_call(
        functools.partial(kernel, (X, Y, Z, H, L, gx, gy, gz)),
        out_shape=(
            jax.ShapeDtypeStruct((X, R, H), BF16),
            jax.ShapeDtypeStruct((1, H), F32),
        ),
        in_specs=[hbm] + [vmem] * 11,
        out_specs=(hbm, vmem),
        scratch_shapes=[
            pltpu.VMEM((X, R, H), BF16),
            pltpu.VMEM((X, R, H), BF16),
            pltpu.VMEM((X, R, H), F32),
            pltpu.VMEM((X + 2, Y * ZP, H), F32),
            pltpu.VMEM((X, R, H), F32),
            pltpu.VMEM((X, R, H), BF16),
            pltpu.VMEM((R, H), F32),
            pltpu.VMEM((R, H), F32),
            pltpu.VMEM((pl.cdiv(NT * NC, 16) * 16, H), F32),
            pltpu.VMEM((L, H, 2 * H), BF16),
            pltpu.VMEM((L, 2 * H, H), BF16),
            pltpu.VMEM((L, H, H), BF16),
            pltpu.VMEM((L, 2, R, H), BF16),
            pltpu.VMEM((L, 2, R, H), BF16),
            pltpu.VMEM((L, 2, X, Z, H), BF16),
            pltpu.VMEM((L, 2, X, Z, H), BF16),
            pltpu.VMEM((L, 2, X, Y, H), BF16),
            pltpu.VMEM((L, 2, X, Y, H), BF16),
            pltpu.VMEM((16, 2 * H), F32),
            pltpu.VMEM((gx * gy, 8, H), F32),
            pltpu.VMEM((gz, 8, H), F32),
            pltpu.SemaphoreType.DMA((X,)),
            pltpu.SemaphoreType.DMA((X,)),
            pltpu.SemaphoreType.DMA((L, 6)),
            pltpu.SemaphoreType.DMA((L, 6)),
            pltpu.SemaphoreType.DMA((2, most)),
            pltpu.SemaphoreType.DMA((2, most)),
        ],
        compiler_params=pltpu.CompilerParams(collective_id=0, has_side_effects=True, vmem_limit_bytes=36 * 2**20),
        name="mesh_step",
    )(
        node_feats.reshape(X, R, H), code, type_table, boundary_table, edge_self, edge_neighbour,
        jnp.transpose(edge_bias, (1, 0, 2)), edge_out, node_self, node_aggregate, node_out, node_gain,
    )
    return latent.reshape(X, Y, Z, H), wall_mean.reshape(H)


def solution(mesh):
    return jax.shard_map(
        per_device,
        mesh=mesh,
        in_specs=(
            P("gx", "gy", "gz", None),
            P("gx", "gy", "gz"),
            P("gx", "gy", "gz"),
            P("gx", "gy", "gz"),
            P(),
            P(),
            P(),
            P(),
            P(),
            P(),
            P(),
            P(),
            P(),
            P(),
        ),
        out_specs=(P("gx", "gy", "gz", None), P()),
        check_vma=False,
    )
```

```python
import functools

import jax
import jax.numpy as jnp
from jax import lax
from jax.experimental import pallas as pl
from jax.experimental.pallas import tpu as pltpu
from jax.sharding import PartitionSpec as P

epsilon = 1e-05
PAD = 8
F32 = jnp.float32
BF16 = jnp.bfloat16


def dot(a, b):
    return jnp.dot(a, b, preferred_element_type=F32)


def gated(u):
    return u * (1.0 + jnp.tanh(u))


def kernel(
    sizes,
    feats, code, *rest,
):
    far, (out, wall_out), held = rest[:10], rest[10:12], rest[12:22]
    (
        fbuf, lat, spart, npart, hsum, hbf, pre, upd, table,
        wcat, wnode, wout,
        xsend, xrecv, ysend, yrecv, zsend, zrecv,
        wall, redxy, redz,
        fsem, wsem, hsend_sem, hrecv_sem, rsend_sem, rrecv_sem,
    ) = rest[22:]
    (
        type_table, boundary_table, edge_self, edge_neighbour, edge_bias, edge_out,
        node_self, node_aggregate, node_out, node_gain,
    ) = held
    X, Y, Z, H, L, gx, gy, gz = sizes
    ZP = Z + 2 * PAD
    R = Y * Z
    counts = {"gx": gx, "gy": gy, "gz": gz}
    me = {a: lax.axis_index(a) for a in counts}

    def load_feats(x):
        return pltpu.make_async_copy(feats.at[x], fbuf.at[x], fsem.at[x])

    loads = [pltpu.make_async_copy(far[i], held[i], wsem.at[i]) for i in range(len(far))]
    for c in loads:
        c.start()
    for x in range(X):
        load_feats(x).start()

    def plane(k):
        return {"gx": lax.rem(me["gx"] + k // gy, gx), "gy": lax.rem(me["gy"] + k % gy, gy)}

    def line(k):
        return {"gz": lax.rem(me["gz"] + k, gz)}

    barrier = pltpu.get_barrier_semaphore()
    peers = [plane(k) for k in range(1, gx * gy)] + [line(k) for k in range(1, gz)]
    total = len(peers)
    for peer in peers:
        pl.semaphore_signal(
            barrier, inc=1, device_id=peer, device_id_type=pl.DeviceIdType.MESH
        )

    for c in loads:
        c.wait()
    for l in range(L):
        wcat[l, :, :H] = (edge_self[l].astype(F32) * 0.5).astype(BF16)
        wcat[l, :, H:] = (edge_neighbour[l].astype(F32) * 0.5).astype(BF16)
        wnode[l, :H] = (node_self[l].astype(F32) * 0.5).astype(BF16)
        wnode[l, H:] = (dot(edge_out[l], node_aggregate[l]) * 0.5).astype(BF16)
        w = node_out[l].astype(F32)
        wout[l] = (w - jnp.mean(w, axis=-1, keepdims=True)).astype(BF16)
    ones = jnp.full((H, H), 1.0 / H, BF16)

    NT, NC = type_table.shape[0], boundary_table.shape[0]
    KT = NT * NC
    KP = table.shape[0]
    table[...] = jnp.zeros_like(table)
    for i in range(NT):
        table[i * NC:(i + 1) * NC] = boundary_table[...] + type_table[i:i + 1]
    t = table[...]
    hi = t.astype(BF16)
    rest = t - hi.astype(F32)
    mid = rest.astype(BF16)
    low = (rest - mid.astype(F32)).astype(BF16)
    table3 = jnp.concatenate([hi, mid, low], axis=0)

    def start_latent(x):
        load_feats(x).wait()
        c = code[x]
        c = jnp.where(c >= KT, c - KT, c)
        rows = lax.broadcasted_iota(jnp.int32, (KP, R), 0)
        hot = jnp.where(rows == c, 1.0, 0.0).astype(BF16)
        hot3 = jnp.concatenate([hot, hot, hot], axis=0)
        extra = lax.dot_general(
            hot3, table3, (((0,), (0,)), ((), ())), preferred_element_type=F32
        )
        lat[x] = (fbuf[x].astype(F32) + extra).astype(BF16)

    def loop(lo, hi, fn):
        def body(i, carry):
            fn(i)
            return carry
        lax.fori_loop(lo, hi, body, 0)

    def halo(l, slot, src, dst, axis, peer):
        return pltpu.make_async_remote_copy(
            src_ref=src,
            dst_ref=dst,
            send_sem=hsend_sem.at[l, slot],
            recv_sem=hrecv_sem.at[l, slot],
            device_id={axis: peer},
            device_id_type=pl.DeviceIdType.MESH,
        )

    up = {a: lax.rem(me[a] + 1, n) for a, n in counts.items()}
    down = {a: lax.rem(me[a] + n - 1, n) for a, n in counts.items()}
    wall[...] = jnp.zeros_like(wall)

    for l in range(L):
        last = l == L - 1
        has_low = me["gy"] > 0
        has_high = me["gy"] < gy - 1
        xs = [
            halo(l, 0, xsend.at[l, 1], xrecv.at[l, 0], "gx", up["gx"]),
            halo(l, 1, xsend.at[l, 0], xrecv.at[l, 1], "gx", down["gx"]),
        ]
        zs = [
            halo(l, 2, zsend.at[l, 1], zrecv.at[l, 0], "gz", up["gz"]),
            halo(l, 3, zsend.at[l, 0], zrecv.at[l, 1], "gz", down["gz"]),
        ]
        y_up = halo(l, 4, ysend.at[l, 1], yrecv.at[l, 0], "gy", up["gy"])
        y_down = halo(l, 5, ysend.at[l, 0], yrecv.at[l, 1], "gy", down["gy"])

        def project(x, face=None, l=l):
            p = dot(lat[x], wcat[l])
            spart[x] = p[:, :H]
            n = p[:, H:]
            for y in range(Y):
                npart[x + 1, y * ZP + PAD:y * ZP + PAD + Z] = n[y * Z:(y + 1) * Z]
            if face is not None:
                xsend[l, face] = n.astype(BF16)
            ysend[l, 0, x] = n[:Z].astype(BF16)
            ysend[l, 1, x] = n[R - Z:].astype(BF16)
            zsend[l, 0, x] = npart[x + 1, pl.ds(PAD, Y, stride=ZP), :].astype(BF16)
            zsend[l, 1, x] = npart[x + 1, pl.ds(PAD + Z - 1, Y, stride=ZP), :].astype(BF16)

        if l == 0:
            start_latent(0)

            def ahead(x):
                project(x)
                start_latent(x + 1)

            project(0, 0)
            start_latent(1)
            loop(1, X - 1, ahead)
            project(X - 1, 1)
            pl.semaphore_wait(barrier, total)
            for c in xs:
                c.start()
        else:
            project(0, 0)
            project(X - 1, 1)
            for c in xs:
                c.start()
            loop(1, X - 1, project)
        pl.when(has_high)(y_up.start)
        pl.when(has_low)(y_down.start)
        for c in zs:
            c.start()

        bias = [(edge_bias[d, l:l + 1] * 0.5).astype(BF16) for d in range(6)]

        def neighbour(x, y, dz=0):
            return npart[x, pl.ds(y * ZP + PAD + dz, Z), :].astype(BF16)

        def edges_xy(x, l=l, bias=bias):
            for y in range(Y):
                rows = slice(y * Z, (y + 1) * Z)
                s = spart[x, rows].astype(BF16)
                h = gated(s + neighbour(x, y) + bias[0]) + gated(s + neighbour(x + 2, y) + bias[1])
                if y > 0:
                    h = h + gated(s + neighbour(x + 1, y - 1) + bias[2])
                if y < Y - 1:
                    h = h + gated(s + neighbour(x + 1, y + 1) + bias[3])
                hsum[x, rows] = h.astype(F32)

        loop(1, X - 1, edges_xy)
        for c in xs:
            c.wait()
        for side, slab in ((0, 0), (1, X + 1)):
            for y in range(Y):
                npart[slab, y * ZP + PAD:y * ZP + PAD + Z] = xrecv[l, side, y * Z:(y + 1) * Z].astype(F32)
        loop(0, 2, lambda i: edges_xy(i * (X - 1)))

        def edge_rows(face, first, d, l=l, bias=bias):
            def add(x):
                rows = slice(first, first + Z)
                u = spart[x, rows] + yrecv[l, face, x].astype(F32) + edge_bias[d, l:l + 1] * 0.5
                hsum[x, rows] = hsum[x, rows] + gated(u)

            loop(0, X, add)

        @pl.when(has_low)
        def _():
            y_up.wait_recv()
            edge_rows(0, 0, 2)

        @pl.when(has_high)
        def _():
            y_down.wait_recv()
            edge_rows(1, R - Z, 3)

        pl.when(has_high)(y_up.wait_send)
        pl.when(has_low)(y_down.wait_send)
        for c in zs:
            c.wait()

        def edges_z(x, l=l, bias=bias):
            npart[x + 1, pl.ds(PAD - 1, Y, stride=ZP), :] = zrecv[l, 0, x].astype(F32)
            npart[x + 1, pl.ds(PAD + Z, Y, stride=ZP), :] = zrecv[l, 1, x].astype(F32)
            for y in range(Y):
                rows = slice(y * Z, (y + 1) * Z)
                s = spart[x, rows].astype(BF16)
                h = gated(s + neighbour(x + 1, y, -1) + bias[4])
                h = h + gated(s + neighbour(x + 1, y, 1) + bias[5])
                hbf[x, rows] = h + hsum[x, rows].astype(BF16)

        gain = node_gain[l:l + 1]

        def first_layer(x, l=l):
            pre[...] = dot(jnp.concatenate([lat[x], hbf[x]], axis=1), wnode[l])

        def second_layer(l=l):
            upd[...] = dot(gated(pre[...]).astype(BF16), wout[l])

        def finish(x, last=last, gain=gain):
            change = upd[...]
            var = dot((change * change).astype(BF16), ones)
            new = lat[x].astype(F32) + change * lax.rsqrt(var + epsilon) * gain
            new = new.astype(BF16)
            (out if last else lat)[x] = new
            if last:
                flag = jnp.where(code[x] >= KT, 1.0, 0.0)
                flag = jnp.broadcast_to(flag, (16, R)).astype(BF16)
                wide = jnp.concatenate([new, jnp.ones((R, H), BF16)], axis=1)
                wall[...] += dot(flag, wide)

        def step(x, edge, one, two, three):
            if three:
                finish(x - 3)
            if two:
                second_layer()
            if one:
                first_layer(x - 1)
            if edge:
                edges_z(x)

        step(0, True, False, False, False)
        step(1, True, True, False, False)
        step(2, True, True, True, False)
        loop(3, X, lambda x, step=step: step(x, True, True, True, True))
        step(X, False, True, True, True)
        step(X + 1, False, False, True, True)
        step(X + 2, False, False, False, True)

    def exchange(part, red, index, mine, count, place):
        red[mine] = part
        copies = []
        for k in range(1, count):
            copies.append(pltpu.make_async_remote_copy(
                src_ref=red.at[mine],
                dst_ref=red.at[mine],
                send_sem=rsend_sem.at[index, k],
                recv_sem=rrecv_sem.at[index, k],
                device_id=place(k),
                device_id_type=pl.DeviceIdType.MESH,
            ))
        for c in copies:
            c.start()
        for c in copies:
            c.wait()
        total = red[0]
        for i in range(1, count):
            total = total + red[i]
        return total

    first = lax.broadcasted_iota(jnp.int32, (8, H), 0) == 0
    part = jnp.where(first, wall[:8, :H], wall[:8, H:])
    part = exchange(part, redxy, 0, me["gx"] * gy + me["gy"], gx * gy, plane)
    part = exchange(part, redz, 1, me["gz"], gz, line)
    wall_out[...] = part[:1] / part[1:2]


def per_device(
    node_feats,
    node_type,
    boundary_code,
    wall_flag,
    type_table,
    boundary_table,
    edge_self,
    edge_neighbour,
    edge_bias,
    edge_out,
    node_self,
    node_aggregate,
    node_out,
    node_gain,
):
    X, Y, Z, H = node_feats.shape
    L = edge_self.shape[0]
    gx, gy, gz = (lax.axis_size(a) for a in ("gx", "gy", "gz"))
    NT, NC = type_table.shape[0], boundary_table.shape[0]
    R, ZP = Y * Z, Z + 2 * PAD
    most = max(gx * gy, gz)
    code = (node_type * NC + boundary_code + wall_flag * (NT * NC)).reshape(X, 1, R)
    vmem = pl.BlockSpec(memory_space=pltpu.VMEM)
    hbm = pl.BlockSpec(memory_space=pltpu.HBM)
    weights = (
        type_table, boundary_table, edge_self, edge_neighbour, jnp.transpose(edge_bias, (1, 0, 2)),
        edge_out, node_self, node_aggregate, node_out, node_gain,
    )
    latent, wall_mean = pl.pallas_call(
        functools.partial(kernel, (X, Y, Z, H, L, gx, gy, gz)),
        out_shape=(
            jax.ShapeDtypeStruct((X, R, H), BF16),
            jax.ShapeDtypeStruct((1, H), F32),
        ),
        in_specs=[hbm, vmem] + [hbm] * 10,
        out_specs=(vmem, vmem),
        scratch_shapes=[pltpu.VMEM(w.shape, w.dtype) for w in weights] + [
            pltpu.VMEM((X, R, H), BF16),
            pltpu.VMEM((X, R, H), BF16),
            pltpu.VMEM((X, R, H), F32),
            pltpu.VMEM((X + 2, Y * ZP, H), F32),
            pltpu.VMEM((X, R, H), F32),
            pltpu.VMEM((X, R, H), BF16),
            pltpu.VMEM((R, H), F32),
            pltpu.VMEM((R, H), F32),
            pltpu.VMEM((pl.cdiv(NT * NC, 16) * 16, H), F32),
            pltpu.VMEM((L, H, 2 * H), BF16),
            pltpu.VMEM((L, 2 * H, H), BF16),
            pltpu.VMEM((L, H, H), BF16),
            pltpu.VMEM((L, 2, R, H), BF16),
            pltpu.VMEM((L, 2, R, H), BF16),
            pltpu.VMEM((L, 2, X, Z, H), BF16),
            pltpu.VMEM((L, 2, X, Z, H), BF16),
            pltpu.VMEM((L, 2, X, Y, H), BF16),
            pltpu.VMEM((L, 2, X, Y, H), BF16),
            pltpu.VMEM((16, 2 * H), F32),
            pltpu.VMEM((gx * gy, 8, H), F32),
            pltpu.VMEM((gz, 8, H), F32),
            pltpu.SemaphoreType.DMA((X,)),
            pltpu.SemaphoreType.DMA((10,)),
            pltpu.SemaphoreType.DMA((L, 6)),
            pltpu.SemaphoreType.DMA((L, 6)),
            pltpu.SemaphoreType.DMA((2, most)),
            pltpu.SemaphoreType.DMA((2, most)),
        ],
        compiler_params=pltpu.CompilerParams(collective_id=0, has_side_effects=True),
        name="mesh_step",
    )(
        node_feats.reshape(X, R, H), code, *weights,
    )
    return latent.reshape(X, Y, Z, H), wall_mean.reshape(H)


def solution(mesh):
    return jax.shard_map(
        per_device,
        mesh=mesh,
        in_specs=(
            P("gx", "gy", "gz", None),
            P("gx", "gy", "gz"),
            P("gx", "gy", "gz"),
            P("gx", "gy", "gz"),
            P(),
            P(),
            P(),
            P(),
            P(),
            P(),
            P(),
            P(),
            P(),
            P(),
        ),
        out_specs=(P("gx", "gy", "gz", None), P()),
        check_vma=False,
    )
```
